32 devices in a mesh: group: 4 (over z), sub: 8 (over y, x, core).
Axes of the slice: x: 2, y: 2, z: 4, core: 2. Of those that a mesh axis runs over, the one named last changes fastest.
Arguments:
- displacement: float32 [3, 35, 32768], P(None, None, ('group', 'sub')), may hold values from -6 to 6
- velocity: float32 [3, 35, 32768], P(None, None, ('group', 'sub')), may hold values from -6 to 6
- geometry_weights: float32 [6, 32768], P(None, ('group', 'sub')), may hold values from 0.2 to 2
- jacobian: float32 [32768], P(('group', 'sub')), may hold values from 0.5 to 2
- strain_map: float32 [630, 105], replicated, may hold values from -0.25 to 0.25
- face_mass: float32 [15, 15], replicated, may hold values from -1 to 2, as said below
- mass_inverse: float32 [35, 35], replicated, may hold values from -1 to 2, as said below
- local_links: int32 [2, 98304], P(None, ('group', 'sub')), may hold values from 0 to 383, as said below
- local_geometry: float32 [4, 98304], P(None, ('group', 'sub')), may hold values from -1 to 3, as said below
- neighbour_links: int32 [2, 4096], P(None, ('group', 'sub')), may hold values from 0 to 2, as said below
- neighbour_geometry: float32 [8, 4096], P(None, ('group', 'sub')), may hold values from -1 to 3, as said below
- cross_links: int32 [6144], P(('group', 'sub')), may hold values from 0 to 2, as said below
- cross_geometry: float32 [4, 6144], P(None, ('group', 'sub')), may hold values from -1 to 3, as said below
Outputs:
- displacement_new: float32 [3, 35, 32768], P(None, None, ('group', 'sub'))
- velocity_new: float32 [3, 35, 32768], P(None, None, ('group', 'sub'))
The draws below stay inside these ranges and needn't reach their ends.
Inputs may be any that keep to these rules, and one draw needn't show every extreme that they name: `local_links`: row 0 is the partner inside the same aligned block of 128 elements, as the steps read it; the pairing is symmetric and never pairs a half-face with itself. Row 1 is the state (0 intact, 1 cohesive, 2 broken), equal on both half-faces of a pair. `local_geometry`: rows 0 to 2 are a unit normal, row 3 a positive scale; both half-faces of a pair hold the same values. `neighbour_links`: row 0: state of the upper shared half-face, row 1: of the lower one (0 intact, 1 cohesive, 2 broken). Row 1 of device (g, s) equals row 0 of the same column on device (g, (s - 1) mod 8). `neighbour_geometry`: rows 0 to 3: unit normal and positive scale of the upper half-face; rows 4 to 7 of device (g, s) equal rows 0 to 3 of the same column on device (g, (s - 1) mod 8). `cross_links`: states (0 intact, 1 cohesive, 2 broken). In the block of 8 slots that a device holds for one partner device, the first count slots hold faces and the rest are padding with state 2; count is the same on both sides of a pair, 1 to 8, 8 for some pair, and the states of matching slots agree. `cross_geometry`: rows 0 to 2 a unit normal, row 3 a positive scale; matching slots of a pair hold the same values. `face_mass`: Symmetric. `mass_inverse`: Symmetric.
All inputs are finite; a program needn't handle non-finite values.
Results may differ from the reference program's by a relative error of at most 0.00011.
Values sent between devices are 32-bit elements; how exact they have to be, the bound alone decides.
No kernel may reach another device: no remote copies, remote signals or barrier semaphores. Data moves between devices by JAX's collectives and lax.ppermute only.
A program may use at most 128 MiB of HBM per device.

```python
import math
import jax
import jax.numpy as jnp
import numpy as np
from jax import lax

COMP = 3
NODES = 35
FNODES = 15
NMAT = 6
SLOT = 8
BLOCK = 128
STEPS = 5
E_DEV = 1024
ELEMS = 32768
F_NB = 128
CROSS = 192
N_GROUP = 4
N_SUB = 8
DEVICES = 32


def face_states(key, shape):
    level = jax.random.randint(key, shape, 0, 8)
    return jnp.where(level < 5, 0, jnp.where(level < 7, 1, 2)).astype(jnp.int32)


def face_geometry(key, count):
    first, second, third = jax.random.split(key, 3)
    height = jax.random.uniform(first, (count,), jnp.float32, -1.0, 1.0)
    azimuth = jax.random.uniform(second, (count,), jnp.float32, -math.pi, math.pi)
    radial = jnp.sqrt(jnp.maximum(1.0 - height * height, 0.0))
    scale = jnp.exp(jax.random.uniform(third, (count,), jnp.float32, math.log(0.3), math.log(3.0)))
    return jnp.stack([radial * jnp.cos(azimuth), radial * jnp.sin(azimuth), height, scale])


def definite(key, order):
    first, second = jax.random.split(key)
    diagonal = jax.random.uniform(first, (order,), jnp.float32, 0.8, 1.2)
    spread = 0.75 / order
    offside = jax.random.uniform(second, (order, order), jnp.float32, -spread, spread)
    offside = 0.5 * (offside + offside.T)
    offside = offside * (1.0 - jnp.eye(order, dtype=jnp.float32))
    return offside + jnp.diag(diagonal)


def draw_face_mass(key, part):
    return definite(jax.random.fold_in(key, 3), FNODES)


def draw_mass_inverse(key, part):
    return definite(jax.random.fold_in(key, 5), NODES)


def local_pairing(key):
    blocks = DEVICES * (E_DEV // BLOCK)
    width = 3 * BLOCK
    scores = jax.random.randint(key, (blocks, width), 0, 1 << 20) * width + jnp.arange(width, dtype=jnp.int32)[None, :]
    order = jnp.argsort(scores, axis=1).astype(jnp.int32)
    swapped = order.reshape(blocks, width // 2, 2)[:, :, ::-1].reshape(blocks, width)
    rows = jnp.arange(blocks, dtype=jnp.int32)[:, None]
    partner = jnp.zeros((blocks, width), jnp.int32).at[rows, order].set(swapped)
    labels = jnp.broadcast_to(jnp.repeat(jnp.arange(width // 2, dtype=jnp.int32), 2)[None, :], (blocks, width))
    pair_index = jnp.zeros((blocks, width), jnp.int32).at[rows, order].set(labels)
    return (partner, pair_index)


def to_columns(blocked):
    leading = blocked.shape[0]
    shaped = blocked.reshape(leading, DEVICES, E_DEV // BLOCK, 3, BLOCK)
    return jnp.transpose(shaped, (0, 1, 3, 2, 4)).reshape(leading, 3 * E_DEV * DEVICES)


def draw_local_links(key, part):
    partner, pair_index = local_pairing(jax.random.fold_in(key, 11))
    blocks = partner.shape[0]
    pair_states = face_states(jax.random.fold_in(key, 12), (blocks, 3 * BLOCK // 2))
    states = jnp.take_along_axis(pair_states, pair_index, axis=1)
    return to_columns(jnp.stack([partner, states])).astype(jnp.int32)


def draw_local_geometry(key, part):
    partner, pair_index = local_pairing(jax.random.fold_in(key, 11))
    blocks = partner.shape[0]
    drawn = face_geometry(jax.random.fold_in(key, 13), blocks * (3 * BLOCK // 2)).reshape(4, blocks, 3 * BLOCK // 2)
    spread = jnp.take_along_axis(drawn, jnp.broadcast_to(pair_index[None], (4, blocks, 3 * BLOCK)), axis=2)
    return to_columns(spread)


def draw_neighbour_links(key, part):
    count = F_NB * DEVICES
    upper_state = face_states(jax.random.fold_in(key, 17), (count,))
    lower_state = jnp.roll(upper_state.reshape(N_GROUP, N_SUB, F_NB), 1, axis=1).reshape(count)
    return jnp.stack([upper_state, lower_state]).astype(jnp.int32)


def draw_neighbour_geometry(key, part):
    count = F_NB * DEVICES
    upper = face_geometry(jax.random.fold_in(key, 19), count)
    lower = jnp.roll(upper.reshape(4, N_GROUP, N_SUB, F_NB), 1, axis=2).reshape(4, count)
    return jnp.concatenate([upper, lower], axis=0)


def to_layout(dense):
    ranks = jnp.arange(DEVICES, dtype=jnp.int32)
    offsets = jnp.arange(N_GROUP - 1, dtype=jnp.int32)
    places = jnp.arange(N_SUB, dtype=jnp.int32)
    groups = ranks // N_SUB
    partners = (groups[:, None, None] + 1 + offsets[None, :, None]) % N_GROUP * N_SUB + places[None, None, :]
    partners = partners.reshape(DEVICES, (N_GROUP - 1) * N_SUB)
    picked = dense[:, ranks[:, None], partners]
    return picked.reshape(dense.shape[0], DEVICES * CROSS)


def draw_cross_links(key, part):
    devices = DEVICES
    keys = jax.random.split(jax.random.fold_in(key, 23), 3)
    lowest = max(1, 3 * SLOT // 8)
    base = jax.random.randint(keys[0], (devices, devices), lowest, SLOT + 1)
    busy = jax.random.randint(keys[1], (devices,), 0, 4) == 0
    counts = jnp.where(busy[:, None] | busy[None, :], base, (base + 1) // 2)
    ranks = jnp.arange(devices, dtype=jnp.int32)
    lower_rank = ranks[:, None] < ranks[None, :]
    counts = jnp.where(lower_rank, counts, counts.T)
    filled = (ranks[:, None] == 0) & (ranks[None, :] == N_SUB) | (ranks[:, None] == N_SUB) & (ranks[None, :] == 0)
    counts = jnp.where(filled, SLOT, counts)
    states = face_states(keys[2], (devices, devices, SLOT))
    states = jnp.where(lower_rank[:, :, None], states, jnp.transpose(states, (1, 0, 2)))
    used = jnp.arange(SLOT, dtype=jnp.int32)[None, None, :] < counts[:, :, None]
    stacked = jnp.where(used, states, 2)[None]
    return to_layout(stacked).reshape(DEVICES * CROSS).astype(jnp.int32)


def draw_cross_geometry(key, part):
    devices = DEVICES
    drawn = face_geometry(jax.random.fold_in(key, 29), devices * devices * SLOT).reshape(4, devices, devices, SLOT)
    ranks = jnp.arange(devices, dtype=jnp.int32)
    lower_rank = (ranks[:, None] < ranks[None, :])[None, :, :, None]
    drawn = jnp.where(lower_rank, drawn, jnp.transpose(drawn, (0, 2, 1, 3)))
    return to_layout(drawn)


def shard_levels(key, dims, cuts, low, high):
    level = 1.0
    for axis_at, shards_of in cuts:
        steps = jax.random.uniform(jax.random.fold_in(jax.random.fold_in(key, 6), axis_at), (shards_of,), jnp.float32, low / len(cuts), high / len(cuts))
        level = level * jnp.repeat(jnp.exp(steps), dims[axis_at] // shards_of).reshape((-1,) + (1,) * (len(dims) - 1 - axis_at))
    return level


def centred(own_key, shape, scale, bound, shards=(), kind=jnp.bfloat16):
    gain = shard_levels(own_key, shape, shards, -0.22, 0.18) if shards else 1.0
    values = jax.random.normal(own_key, shape, jnp.float32) * scale * gain
    return jnp.minimum(jnp.maximum(values, -bound), bound).astype(kind)


def setup_inputs(seed: int = 0) -> dict:
    key_of = jax.random.split(jax.random.key(seed), 14)
    return {
        "displacement": centred(key_of[0], (COMP, NODES, ELEMS), 1.0, 6.0, ((2, 32),), jnp.float32),
        "velocity": centred(key_of[1], (COMP, NODES, ELEMS), 1.0, 6.0, ((2, 32),), jnp.float32),
        "geometry_weights": jnp.clip(jnp.exp(math.log(2.0) - 2.3025851 * jax.random.uniform(key_of[2], (NMAT, ELEMS), jnp.float32) ** shard_levels(key_of[2], (NMAT, ELEMS), ((1, 32),), -0.2, 0.2)), 0.2, 2.0),
        "jacobian": jnp.clip(jnp.exp(math.log(2.0) - 1.3862944 * jax.random.uniform(key_of[3], (ELEMS,), jnp.float32) ** shard_levels(key_of[3], (ELEMS,), ((0, 32),), -0.2, 0.2)), 0.5, 2.0),
        "strain_map": centred(key_of[4], (NMAT * COMP * NODES, COMP * NODES), (NMAT * COMP * NODES) ** -0.5, 0.25, (), jnp.float32),
        "face_mass": draw_face_mass(jax.random.fold_in(key_of[13], 71), 0),
        "mass_inverse": draw_mass_inverse(jax.random.fold_in(key_of[13], 71), 0),
        "local_links": draw_local_links(jax.random.fold_in(key_of[13], 71), 0),
        "local_geometry": draw_local_geometry(jax.random.fold_in(key_of[13], 71), 0),
        "neighbour_links": draw_neighbour_links(jax.random.fold_in(key_of[13], 71), 0),
        "neighbour_geometry": draw_neighbour_geometry(jax.random.fold_in(key_of[13], 71), 0),
        "cross_links": draw_cross_links(jax.random.fold_in(key_of[13], 71), 0),
        "cross_geometry": draw_cross_geometry(jax.random.fold_in(key_of[13], 71), 0),
    }


shear_weight = 0.5
opening_scale = 4.0
time_step = 0.25
highest = lax.Precision.HIGHEST


def face_table():
    points = [(first, second, third, 4 - first - second - third) for first in range(5) for second in range(5 - first) for third in range(5 - first - second)]
    result = np.zeros((4, 15, 35), np.float32)
    for side in range(4):
        members = [index for index, point in enumerate(points) if point[side] == 0]
        for place, index in enumerate(members):
            result[side, place, index] = 1.0
    return result


def cohesive_traction(jump, normal, state):
    along = jnp.sum(normal[:, None, :] * jump, axis=0)
    normal_part = along[None] * normal[:, None, :]
    tangent = jump - normal_part
    opening = along * along + shear_weight * jnp.sum(tangent * tangent, axis=0)
    softened = jnp.exp(-opening / opening_scale)[None] * (normal_part + shear_weight * tangent)
    zeros = jnp.zeros_like(jump)
    return jnp.where(state[None, None, :] == 0, jump, jnp.where(state[None, None, :] == 1, softened, zeros))


def face_force(jump, geometry, state, face_mass):
    traction = cohesive_traction(jump, geometry[0:3], state)
    spread = jnp.einsum("ij,cjf->cif", face_mass, traction, precision=highest)
    return geometry[3][None, None, :] * spread


def flatten(array):
    return array.reshape(COMP, FNODES, -1)


def reference(displacement, velocity, geometry_weights, jacobian, strain_map, face_mass, mass_inverse, local_links, local_geometry, neighbour_links, neighbour_geometry, cross_links, cross_geometry):
    table = jnp.asarray(face_table())
    count_blocks = E_DEV // BLOCK
    partner = jnp.transpose(local_links[0].reshape(DEVICES, 3, count_blocks, BLOCK), (0, 2, 1, 3)).reshape(DEVICES * count_blocks, 3 * BLOCK)
    partner = jnp.broadcast_to(partner[None, None], (COMP, FNODES, DEVICES * count_blocks, 3 * BLOCK)).astype(jnp.int32)
    groups_at = jnp.arange(N_GROUP, dtype=jnp.int32)[:, None, None, None]
    places_at = jnp.arange(N_SUB, dtype=jnp.int32)[None, :, None, None]
    offsets_at = jnp.arange(N_GROUP - 1, dtype=jnp.int32)[None, None, :, None]
    targets_at = jnp.arange(N_SUB, dtype=jnp.int32)[None, None, None, :]
    other_group = (groups_at + 1 + offsets_at) % N_GROUP
    other_block = N_GROUP - 2 - offsets_at
    spare = E_DEV - 2 * F_NB - CROSS
    field = displacement
    for step in range(STEPS):
        traces = jnp.einsum("kin,cne->cike", table, field, precision=highest)
        own_local = jnp.transpose(traces[:, :, 1:].reshape(COMP, FNODES, 3, DEVICES, E_DEV), (0, 1, 3, 2, 4))
        blocked = jnp.transpose(own_local.reshape(COMP, FNODES, DEVICES, 3, count_blocks, BLOCK), (0, 1, 2, 4, 3, 5)).reshape(COMP, FNODES, DEVICES * count_blocks, 3 * BLOCK)
        paired = jnp.take_along_axis(blocked, partner, axis=3)
        paired = jnp.transpose(paired.reshape(COMP, FNODES, DEVICES, count_blocks, 3, BLOCK), (0, 1, 2, 4, 3, 5)).reshape(COMP, FNODES, DEVICES * 3 * E_DEV)
        local_force = face_force(paired - own_local.reshape(COMP, FNODES, DEVICES * 3 * E_DEV), local_geometry, local_links[1], face_mass)
        local_force = jnp.transpose(local_force.reshape(COMP, FNODES, DEVICES, 3, E_DEV), (0, 1, 3, 2, 4)).reshape(COMP, FNODES, 3, ELEMS)
        rim = traces[:, :, 0].reshape(COMP, FNODES, N_GROUP, N_SUB, E_DEV)
        upper = rim[..., 0:F_NB]
        lower = rim[..., F_NB:2 * F_NB]
        crossing = rim[..., 2 * F_NB:2 * F_NB + CROSS].reshape(COMP, FNODES, N_GROUP, N_SUB, N_GROUP - 1, N_SUB, SLOT)
        upper_force = face_force(flatten(jnp.roll(lower, -1, axis=3) - upper), neighbour_geometry[0:4], neighbour_links[0], face_mass)
        lower_force = face_force(flatten(jnp.roll(upper, 1, axis=3) - lower), neighbour_geometry[4:8], neighbour_links[1], face_mass)
        facing = crossing[:, :, other_group, targets_at, other_block, places_at, :]
        cross_force = face_force(flatten(facing - crossing), cross_geometry, cross_links, face_mass)
        shape = (COMP, FNODES, N_GROUP, N_SUB, -1)
        filler = jnp.zeros((COMP, FNODES, N_GROUP, N_SUB, spare), field.dtype)
        rim_force = jnp.concatenate([upper_force.reshape(shape), lower_force.reshape(shape), cross_force.reshape(shape), filler], axis=4).reshape(COMP, FNODES, ELEMS)
        forces = jnp.concatenate([rim_force[:, :, None], local_force], axis=2)
        face_load = jnp.einsum("kin,cike->cne", table, forces, precision=highest)
        strain = jnp.dot(strain_map, field.reshape(COMP * NODES, ELEMS), precision=highest)
        weighted = (strain.reshape(NMAT, COMP * NODES, ELEMS) * geometry_weights[:, None, :]).reshape(NMAT * COMP * NODES, ELEMS)
        volume = -jnp.dot(strain_map.T, weighted, precision=highest).reshape(COMP, NODES, ELEMS)
        acceleration = jnp.einsum("nm,cme->cne", mass_inverse, volume + face_load, precision=highest) / jacobian[None, None, :]
        velocity = velocity + time_step * acceleration
        field = field + time_step * velocity
    return field, velocity
```

```python
import functools
import math

import jax
import jax.numpy as jnp
import numpy as np
from jax import lax
from jax.experimental import pallas as pl
from jax.experimental.pallas import tpu as pltpu
from jax.sharding import PartitionSpec as P

BLOCK = 128
PAD = 40
ROWS = 128
FACE = 16
TRACE = 3 * FACE
TILE = 256

shear_weight = 0.5
opening_scale = 4.0
time_step = 0.25
highest = lax.Precision.HIGHEST
bf16 = jnp.bfloat16
f32 = jnp.float32


def face_table():
    points = [
        (first, second, third, 4 - first - second - third)
        for first in range(5)
        for second in range(5 - first)
        for third in range(5 - first - second)
    ]
    result = np.zeros((4, 15, 35), np.float32)
    for side in range(4):
        members = [index for index, point in enumerate(points) if point[side] == 0]
        for place, index in enumerate(members):
            result[side, place, index] = 1.0
    return result


def tables():
    table = face_table()
    nodes = table.shape[2]
    spread = np.zeros((3 * nodes, ROWS), np.float32)
    rows = np.zeros((ROWS, nodes), np.float32)
    for c in range(3):
        for n in range(nodes):
            spread[c * nodes + n, c * PAD + n] = 1.0
            rows[c * PAD + n, n] = 1.0
    place = np.zeros((3 * TRACE, 15), np.float32)
    lift = np.zeros((ROWS, 3 * TRACE), np.float32)
    lift0 = np.zeros((ROWS, TRACE), np.float32)
    for c in range(3):
        for i in range(15):
            for k in range(3):
                place[k * TRACE + c * FACE + i, i] = 1.0
                for n in range(nodes):
                    lift[c * PAD + n, k * TRACE + c * FACE + i] = table[k + 1, i, n]
            for n in range(nodes):
                lift0[c * PAD + n, c * FACE + i] = table[0, i, n]
    pick = np.concatenate([lift.T, lift.T], axis=1)
    return spread, rows, place, lift, lift0, pick


def dot(a, b):
    return lax.dot_general(a, b, (((1,), (0,)), ((), ())), preferred_element_type=f32)


def dot_full(a, b):
    return lax.dot_general(
        a, b, (((1,), (0,)), ((), ())), precision=highest, preferred_element_type=f32
    )


def dot_full_t(a, b):
    return lax.dot_general(
        a, b, (((1,), (1,)), ((), ())), precision=highest, preferred_element_type=f32
    )


def pieces(value):
    high = value.astype(bf16)
    low = (value - high.astype(f32)).astype(bf16)
    return high, low


def traction(jump, normal, weight0, weight1):
    j0, j1, j2 = jump
    n0, n1, n2 = normal
    along = n0 * j0 + n1 * j1 + n2 * j2
    t0, t1, t2 = j0 - along * n0, j1 - along * n1, j2 - along * n2
    opening = along * along + shear_weight * (t0 * t0 + t1 * t1 + t2 * t2)
    beta = weight1 * jnp.exp(opening * (-1.0 / opening_scale))
    alpha = weight0 + beta
    gamma = beta * along
    return [alpha * j0 + gamma * n0, alpha * j1 + gamma * n1, alpha * j2 + gamma * n2]


def build_inner(links, geometry, weights, jac, coef, index):
    inverse = 1.0 / jac
    for q in range(3):
        geo = geometry(q)
        link = links(q)
        partner = link[0:1, :]
        state = link[1:2, :]
        scale = geo[3:4, :] * inverse
        coef[5 * q : 5 * q + 3, :] = geo[0:3, :]
        coef[5 * q + 3 : 5 * q + 4, :] = jnp.where(state == 0, scale, 0.0)
        coef[5 * q + 4 : 5 * q + 5, :] = jnp.where(state == 1, (1.0 - shear_weight) * scale, 0.0)
        index[q : q + 1, :] = lax.bitwise_and(partner, BLOCK - 1)
        index[3 + q : 4 + q, :] = lax.div(partner, BLOCK)
    count = weights.shape[0]
    coef[15 : 15 + count, :] = weights * inverse


def local_change(field, at, coef, index, ops):
    high_op, low_op, pick, lift = ops
    lanes = pl.ds(at, TILE)
    high, low = pieces(field[:, lanes])
    both = jnp.concatenate([high, low], axis=0)
    total = None
    for m in range(high_op.shape[0]):
        part = dot(high_op[m], both) + dot(low_op[m], both)
        part = part * coef[15 + m : 16 + m, lanes]
        total = part if total is None else total + part
    traces = dot(pick[...], both)
    halves = []
    for half in range(TILE // BLOCK):
        start = at + half * BLOCK
        part = traces[:, half * BLOCK : (half + 1) * BLOCK]
        forces = []
        for q in range(3):
            where = jnp.broadcast_to(index[q : q + 1, pl.ds(start, BLOCK)], (TRACE, BLOCK))
            side = index[3 + q : 4 + q, pl.ds(start, BLOCK)]
            found = [
                jnp.take_along_axis(
                    part[k * TRACE : (k + 1) * TRACE], where, axis=1, mode="promise_in_bounds"
                )
                for k in range(3)
            ]
            paired = jnp.where(side == 0, found[0], jnp.where(side == 1, found[1], found[2]))
            jump = paired - part[q * TRACE : (q + 1) * TRACE]
            rows = [coef[5 * q + r : 5 * q + r + 1, pl.ds(start, BLOCK)] for r in range(5)]
            forces += traction(
                [jump[c * FACE : (c + 1) * FACE] for c in range(3)], rows[0:3], rows[3], rows[4]
            )
        halves.append(jnp.concatenate(forces, axis=0))
    high, low = pieces(jnp.concatenate(halves, axis=1))
    first = dot(lift[...], high)
    second = dot(lift[0:ROWS, :], low)
    return total + (first[0:ROWS] + first[ROWS : 2 * ROWS] + second)


def load_state(source, target):
    target[...] = jnp.zeros_like(target)
    for c in range(3):
        target[c * PAD : c * PAD + source.shape[1], :] = source[c]


def trace_of(field, lanes):
    return [field[c * PAD : c * PAD + FACE, lanes] for c in range(3)]


def pack(first, second, extra, shared, groups, places, upper, lower, cross):
    parts = [first]
    if second is not None:
        parts.append(second)
    if extra is not None:
        parts.append(extra)
    rows = jnp.concatenate(parts, axis=0)
    upper[...] = rows[:, 0:shared]
    lower[...] = rows[:, shared : 2 * shared]
    rest = rows[:, 2 * shared :]
    missing = BLOCK - rest.shape[0]
    rest = jnp.concatenate([rest, jnp.zeros((missing, rest.shape[1]), f32)], axis=0)
    blocks = rest.T.reshape(rest.shape[1] // 8, 8, BLOCK)
    group = lax.axis_index("group")
    cross[pl.ds(group * places, places)] = jnp.zeros((places, 8, BLOCK), f32)
    for b in range(groups - 1):
        target = lax.rem(group + (1 + b), groups)
        cross[pl.ds(target * places, places)] = blocks[b * places : (b + 1) * places]


def unpack(upper, lower, cross, groups, places, width):
    group = lax.axis_index("group")
    parts = []
    for b in range(groups - 1):
        source = lax.rem(group + (1 + b), groups)
        parts.append(cross[pl.ds(source * places, places)].reshape(places * 8, BLOCK))
    spare = width - (groups - 1) * places * 8
    if spare:
        parts.append(jnp.zeros((spare, BLOCK), f32))
    slots = jnp.concatenate(parts, axis=0).T
    return jnp.concatenate([upper[...], lower[...], slots[0 : upper.shape[0]]], axis=1)


def split_rows(value):
    return [value[c * FACE : (c + 1) * FACE] for c in range(3)]


def rim_traction(jump, rim):
    rows = [rim[r : r + 1, :] for r in range(5)]
    return jnp.concatenate(traction(split_rows(jump), rows[0:3], rows[3], rows[4]), axis=0)


def times_lift0(lift0, value):
    high, low = pieces(value)
    return dot(lift0[...], jnp.concatenate([high, low, high], axis=0))


def first_pack(sizes, disp, jac, upper, lower, cross):
    shared, groups, places, rim_lanes = sizes
    trace = jnp.concatenate([disp[c, 0:FACE, :] for c in range(3)], axis=0)
    extra = jnp.broadcast_to(1.0 / jac[:, 0:rim_lanes], (8, rim_lanes))
    pack(trace, None, extra, shared, groups, places, upper, lower, cross)


def prepare(
    sizes,
    strain,
    face_mass,
    mass_inverse,
    spread,
    rows,
    place,
    lift,
    lift0,
    high_op,
    low_op,
    lift_op,
    lift0_op,
    trace_op,
):
    size = strain.shape[1]
    row = lax.broadcasted_iota(jnp.int32, (ROWS, ROWS), 0)
    col = lax.broadcasted_iota(jnp.int32, (ROWS, ROWS), 1)
    inverse = dot_full_t(dot_full(rows[...], mass_inverse[...]), rows[...])
    inverse = jnp.where(lax.div(row, PAD) == lax.div(col, PAD), inverse, 0.0)
    inverse = inverse * (time_step * time_step)
    for m in range(high_op.shape[0]):
        block = dot_full(strain[m * size : (m + 1) * size, :], spread[...])
        value = -dot_full(dot_full_t(inverse, block), block)
        high, low = pieces(value)
        high_op[m] = jnp.concatenate([high, high], axis=1)
        low_op[m] = jnp.concatenate([low, low], axis=1)
    wide = 3 * TRACE
    row = lax.broadcasted_iota(jnp.int32, (wide, wide), 0)
    col = lax.broadcasted_iota(jnp.int32, (wide, wide), 1)
    mass = dot_full_t(dot_full(place[...], face_mass[...]), place[...])
    same = lax.rem(lax.div(row, FACE), 3) == lax.rem(lax.div(col, FACE), 3)
    mass = jnp.where(same, mass, 0.0)
    inner = jnp.where(lax.div(row, TRACE) == lax.div(col, TRACE), mass, 0.0)
    value = dot_full(inverse, dot_full(lift[...], inner))
    high, low = pieces(value)
    lift_op[0:ROWS, :] = high
    lift_op[ROWS : 2 * ROWS, :] = low
    value = dot_full(inverse, dot_full(lift0[...], mass[0:TRACE, :]))

    def three(value):
        high = value.astype(bf16).astype(f32)
        col = lax.broadcasted_iota(jnp.int32, value.shape, 1)
        return jnp.where(col < 2 * TRACE, high, value - high).astype(bf16)

    lift0_op[...] = three(value)
    trace_op[...] = three(
        jnp.concatenate([value[c * PAD : c * PAD + FACE] for c in range(3)], axis=0)
    )


def start_rim(
    sizes,
    disp,
    vel,
    links,
    geometry,
    weights,
    jac,
    next_links,
    next_geometry,
    cross_links,
    cross_geometry,
    high_op,
    low_op,
    pick,
    lift_op,
    field_out,
    vel_out,
    coef,
    index,
    rim,
):
    shared, groups, places, lanes = sizes
    elements = links.shape[1] // 3
    inverse = jac[:, 0:lanes]
    build_inner(
        lambda q: links[:, q * elements : q * elements + lanes],
        lambda q: geometry[:, q * elements : q * elements + lanes],
        weights[:, 0:lanes],
        inverse,
        coef,
        index,
    )
    rim[...] = jnp.zeros_like(rim)
    slots = cross_links.shape[1]
    for at, count, geo, state in (
        (0, shared, next_geometry[0:4, :], next_links[0:1, :]),
        (shared, shared, next_geometry[4:8, :], next_links[1:2, :]),
        (2 * shared, slots, cross_geometry[...], cross_links[...]),
    ):
        rim[0:3, at : at + count] = geo[0:3, :]
        rim[3:4, at : at + count] = jnp.where(state == 0, 1.0, 0.0)
        rim[4:5, at : at + count] = jnp.where(state == 1, 1.0 - shear_weight, 0.0)
        rim[6:7, at : at + count] = geo[3:4, :]
    rim[5:6, :] = rim[6:7, :] * (1.0 / inverse)
    load_state(disp, field_out)
    load_state(vel, vel_out)
    ops = (high_op, low_op, pick, lift_op)
    for at in range(0, lanes, TILE):
        span = pl.ds(at, TILE)
        vel_out[:, span] = time_step * vel_out[:, span] + local_change(
            field_out, at, coef, index, ops
        )


def first_step(
    sizes,
    upper_in,
    lower_in,
    cross_in,
    field,
    vel,
    coef,
    index,
    rim,
    high_op,
    low_op,
    pick,
    lift_op,
    lift0_op,
    field_out,
    vel_out,
    own_out,
    rim_out,
    upper,
    lower,
    cross,
):
    shared, groups, places, lanes = sizes
    every = slice(None)
    arrived = unpack(upper_in, lower_in, cross_in, groups, places, lanes - 2 * shared)
    own = jnp.concatenate(trace_of(field, every), axis=0)
    pull = rim_traction(arrived[0:TRACE] - own, rim)
    rim_out[0:6, :] = rim[0:6, :]
    rim_out[6:7, :] = rim[5:6, :] + rim[6:7, :] * arrived[TRACE : TRACE + 1]
    rim_out[7:8, :] = rim[7:8, :]
    change = times_lift0(lift0_op, pull * rim[5:6, :])
    speed = vel[...] + change
    vel_out[...] = speed
    field_out[...] = field[...] + speed
    send_two(sizes, field_out, vel_out, own_out, coef, index, (high_op, low_op, pick, lift_op), upper, lower, cross)


def send_two(sizes, field_out, vel_out, own_out, coef, index, ops, upper, lower, cross):
    shared, groups, places, lanes = sizes
    every = slice(None)
    first = jnp.concatenate(trace_of(field_out, every), axis=0)
    own_out[...] = first
    for at in range(0, lanes, TILE):
        span = pl.ds(at, TILE)
        speed = vel_out[:, span] + local_change(field_out, at, coef, index, ops)
        vel_out[:, span] = speed
        field_out[:, span] = field_out[:, span] + speed
    second = jnp.concatenate(trace_of(field_out, every), axis=0)
    pack(first, second, None, shared, groups, places, upper, lower, cross)


def take_two(sizes, upper_in, lower_in, cross_in, field, vel, own, coef, index, rim, ops, lift0_op, trace_op, field_out, vel_out):
    shared, groups, places, lanes = sizes
    every = slice(None)
    arrived = unpack(upper_in, lower_in, cross_in, groups, places, lanes - 2 * shared)
    pull = rim_traction(arrived[0:TRACE] - own[...], rim)
    later = arrived[TRACE : 2 * TRACE] - jnp.concatenate(trace_of(field, every), axis=0)
    later = later - times_lift0(trace_op, pull * rim[6:7, :])
    pull_later = rim_traction(later, rim)
    change = times_lift0(lift0_op, pull * rim[5:6, :])
    vel_out[...] = vel[...] + change
    field_out[...] = field[...] + change
    change = times_lift0(lift0_op, pull_later * rim[5:6, :])
    for at in range(0, lanes, TILE):
        span = pl.ds(at, TILE)
        speed = vel_out[:, span] + (
            local_change(field_out, at, coef, index, ops) + change[:, at : at + TILE]
        )
        vel_out[:, span] = speed
        field_out[:, span] = field_out[:, span] + speed


def middle_steps(
    sizes,
    upper_in,
    lower_in,
    cross_in,
    field,
    vel,
    own,
    coef,
    index,
    rim,
    high_op,
    low_op,
    pick,
    lift_op,
    lift0_op,
    trace_op,
    field_out,
    vel_out,
    own_out,
    upper,
    lower,
    cross,
):
    ops = (high_op, low_op, pick, lift_op)
    take_two(sizes, upper_in, lower_in, cross_in, field, vel, own, coef, index, rim, ops, lift0_op, trace_op, field_out, vel_out)
    send_two(sizes, field_out, vel_out, own_out, coef, index, ops, upper, lower, cross)


def last_steps(
    sizes,
    upper_in,
    lower_in,
    cross_in,
    field,
    vel,
    own,
    coef,
    index,
    rim,
    high_op,
    low_op,
    pick,
    lift_op,
    lift0_op,
    trace_op,
    *rest,
):
    disp_out, vel_out, field_new, vel_new = rest[-4:]
    ops = (high_op, low_op, pick, lift_op)
    take_two(sizes, upper_in, lower_in, cross_in, field, vel, own, coef, index, rim, ops, lift0_op, trace_op, field_new, vel_new)
    store_state(field_new, vel_new, disp_out, vel_out)


def store_state(field, vel, disp_out, vel_out):
    for c in range(3):
        nodes = disp_out.shape[1]
        disp_out[c] = field[c * PAD : c * PAD + nodes, :]
        vel_out[c] = (1.0 / time_step) * vel[c * PAD : c * PAD + nodes, :]


def inside(
    steps,
    disp,
    vel,
    link1,
    link2,
    link3,
    geo1,
    geo2,
    geo3,
    weights,
    jac,
    high_op,
    low_op,
    pick,
    lift_op,
    disp_out,
    vel_out,
    field,
    speed,
    coef,
    index,
):
    links = (link1, link2, link3)
    geos = (geo1, geo2, geo3)
    build_inner(
        lambda q: links[q][...], lambda q: geos[q][...], weights[...], jac[...], coef, index
    )
    load_state(disp, field)
    load_state(vel, speed)
    speed[...] = time_step * speed[...]
    ops = (high_op, low_op, pick, lift_op)

    def step(_, carry):
        for at in range(0, field.shape[1], TILE):
            span = pl.ds(at, TILE)
            new = speed[:, span] + local_change(field, at, coef, index, ops)
            speed[:, span] = new
            field[:, span] = field[:, span] + new
        return carry

    lax.fori_loop(0, steps, step, 0)
    store_state(field, speed, disp_out, vel_out)


def struct(shape, dtype=f32):
    return jax.ShapeDtypeStruct(shape, dtype)


def cost(flops):
    return pl.CostEstimate(flops=flops, bytes_accessed=1 << 20, transcendentals=0)


def shifted(value, axis, steps):
    count = lax.axis_size(axis)
    pairs = [(source, (source + steps) % count) for source in range(count)]
    return lax.ppermute(value, axis, pairs)


def exchange(upper, lower, cross):
    mixed = lax.all_to_all(cross, ("group", "sub"), 0, 0, tiled=True)
    return shifted(lower, "sub", -1), shifted(upper, "sub", 1), mixed


def shards(
    displacement,
    velocity,
    geometry_weights,
    jacobian,
    strain_map,
    face_mass,
    mass_inverse,
    local_links,
    local_geometry,
    neighbour_links,
    neighbour_geometry,
    cross_links,
    cross_geometry,
):
    components, nodes, elements = displacement.shape
    count = geometry_weights.shape[0]
    groups = lax.axis_size("group")
    places = lax.axis_size("sub")
    slots = cross_links.shape[0]
    shared = neighbour_links.shape[1]
    lanes = math.ceil((2 * shared + slots) / TILE) * TILE
    sizes = (shared, groups, places, lanes)
    spread, rows, place, lift, lift0, pick = (jnp.asarray(t) for t in tables())
    pick = pick.astype(bf16)
    jac = jacobian.reshape(1, elements)
    cross_row = cross_links.reshape(1, slots)
    state_shape = struct((ROWS, lanes))
    vmem = pl.BlockSpec(memory_space=pltpu.VMEM)
    part = pl.BlockSpec((components, nodes, lanes), lambda i: (0, 0, 0))
    devices = groups * places

    def messages(height):
        return (struct((height, shared)), struct((height, shared)), struct((devices, 8, BLOCK)))

    sends = pl.pallas_call(
        functools.partial(first_pack, sizes),
        grid=(1,),
        out_shape=messages(TRACE + 8),
        in_specs=[part, vmem],
        cost_estimate=cost(1 << 20),
        name="first_pack",
    )(displacement, jac)
    arrived = exchange(*sends)

    high_op, low_op, lift_op, lift0_op, trace_op = pl.pallas_call(
        functools.partial(prepare, sizes),
        out_shape=(
            struct((count, ROWS, 2 * ROWS), bf16),
            struct((count, ROWS, 2 * ROWS), bf16),
            struct((2 * ROWS, 3 * TRACE), bf16),
            struct((ROWS, 3 * TRACE), bf16),
            struct((TRACE, 3 * TRACE), bf16),
        ),
        cost_estimate=cost(1 << 24),
        name="prepare",
    )(strain_map, face_mass, mass_inverse, spread, rows, place, lift, lift0)

    field, vel, coef, index, rim = pl.pallas_call(
        functools.partial(start_rim, sizes),
        grid=(1,),
        out_shape=(
            state_shape,
            state_shape,
            struct((24, lanes)),
            struct((8, lanes), jnp.int32),
            struct((8, lanes)),
        ),
        in_specs=[part, part] + [vmem] * 12,
        cost_estimate=cost(1 << 24),
        name="start_rim",
    )(
        displacement,
        velocity,
        local_links,
        local_geometry,
        geometry_weights,
        jac,
        neighbour_links,
        neighbour_geometry,
        cross_row,
        cross_geometry,
        high_op,
        low_op,
        pick,
        lift_op,
    )

    field, vel, own, rim, *sends = pl.pallas_call(
        functools.partial(first_step, sizes),
        out_shape=(state_shape, state_shape, struct((TRACE, lanes)), struct((8, lanes)))
        + messages(2 * TRACE),
        cost_estimate=cost(1 << 24),
        name="first_step",
    )(*arrived, field, vel, coef, index, rim, high_op, low_op, pick, lift_op, lift0_op)
    arrived = exchange(*sends)

    inner = elements - lanes
    outputs = []
    if inner:
        width = math.gcd(lanes, inner)
        skip = lanes // width
        per_face = elements // width
        piece = pl.BlockSpec((components, nodes, width), lambda i: (0, 0, skip + i))

        def columns(height, q=0):
            return pl.BlockSpec((height, width), lambda i: (0, q * per_face + skip + i))

        outputs = pl.pallas_call(
            functools.partial(inside, 5),
            grid=(inner // width,),
            out_shape=(struct(displacement.shape), struct(displacement.shape)),
            in_specs=[piece, piece]
            + [columns(2, q) for q in range(3)]
            + [columns(4, q) for q in range(3)]
            + [columns(count), columns(1)]
            + [vmem] * 4,
            out_specs=(piece, piece),
            scratch_shapes=[
                pltpu.VMEM((ROWS, width), f32),
                pltpu.VMEM((ROWS, width), f32),
                pltpu.VMEM((24, width), f32),
                pltpu.VMEM((8, width), jnp.int32),
            ],
            cost_estimate=cost(1 << 26),
            name="inside",
        )(
            displacement,
            velocity,
            *[local_links] * 3,
            *[local_geometry] * 3,
            geometry_weights,
            jac,
            high_op,
            low_op,
            pick,
            lift_op,
        )

    field, vel, own, *sends = pl.pallas_call(
        functools.partial(middle_steps, sizes),
        out_shape=(state_shape, state_shape, struct((TRACE, lanes))) + messages(2 * TRACE),
        cost_estimate=cost(1 << 24),
        name="middle_steps",
    )(*arrived, field, vel, own, coef, index, rim, high_op, low_op, pick, lift_op, lift0_op, trace_op)
    arrived = exchange(*sends)

    anywhere = pl.BlockSpec(memory_space=pl.ANY)
    return pl.pallas_call(
        functools.partial(last_steps, sizes),
        grid=(1,),
        out_shape=(struct(displacement.shape), struct(displacement.shape)),
        in_specs=[vmem] * 15 + [anywhere] * len(outputs),
        out_specs=(part, part),
        scratch_shapes=[pltpu.VMEM((ROWS, lanes), f32), pltpu.VMEM((ROWS, lanes), f32)],
        input_output_aliases={15: 0, 16: 1} if inner else {},
        cost_estimate=cost(1 << 24),
        name="last_steps",
    )(*arrived, field, vel, own, coef, index, rim, high_op, low_op, pick, lift_op, lift0_op, trace_op, *outputs)


def solution(mesh):
    return jax.shard_map(
        shards,
        mesh=mesh,
        in_specs=(
            P(None, None, ("group", "sub")),
            P(None, None, ("group", "sub")),
            P(None, ("group", "sub")),
            P(("group", "sub")),
            P(),
            P(),
            P(),
            P(None, ("group", "sub")),
            P(None, ("group", "sub")),
            P(None, ("group", "sub")),
            P(None, ("group", "sub")),
            P(("group", "sub")),
            P(None, ("group", "sub")),
        ),
        out_specs=(P(None, None, ("group", "sub")), P(None, None, ("group", "sub"))),
        check_vma=False,
    )
```

```python
import functools
import math

import jax
import jax.numpy as jnp
import numpy as np
from jax import lax
from jax.experimental import pallas as pl
from jax.experimental.pallas import tpu as pltpu
from jax.sharding import PartitionSpec as P

BLOCK = 128
PAD = 40
ROWS = 3 * PAD
DEPTH = 128
FACE = 16
TRACE = 3 * FACE
TILE = 256
VMEM_LIMIT = 20 << 20

shear_weight = 0.5
opening_scale = 4.0
time_step = 0.25
highest = lax.Precision.HIGHEST
bf16 = jnp.bfloat16
f32 = jnp.float32


def face_table():
    points = [
        (first, second, third, 4 - first - second - third)
        for first in range(5)
        for second in range(5 - first)
        for third in range(5 - first - second)
    ]
    result = np.zeros((4, 15, 35), np.float32)
    for side in range(4):
        members = [index for index, point in enumerate(points) if point[side] == 0]
        for place, index in enumerate(members):
            result[side, place, index] = 1.0
    return result


def tables():
    table = face_table()
    nodes = table.shape[2]
    place = np.zeros((9 * TRACE, 15), np.float32)
    lift = np.zeros((ROWS, 3 * TRACE), np.float32)
    lift0 = np.zeros((ROWS, TRACE), np.float32)
    for c in range(3):
        for i in range(15):
            for k in range(9):
                place[k * TRACE + c * FACE + i, i] = 1.0
            for n in range(nodes):
                for k in range(3):
                    lift[c * PAD + n, k * TRACE + c * FACE + i] = table[k + 1, i, n]
                lift0[c * PAD + n, c * FACE + i] = table[0, i, n]
    pick = np.zeros((3 * TRACE, 2 * DEPTH), np.float32)
    pick[:, 0:ROWS] = lift.T
    pick[:, DEPTH : DEPTH + ROWS] = lift.T
    return place, lift, lift0, pick


def dot(a, b):
    return lax.dot_general(a, b, (((1,), (0,)), ((), ())), preferred_element_type=f32)


def dot_t(a, b):
    return lax.dot_general(a, b, (((1,), (1,)), ((), ())), preferred_element_type=f32)


def pieces(value):
    high = value.astype(bf16)
    low = (value - high.astype(f32)).astype(bf16)
    return high, low


def dot_pieces(a, b, product=dot):
    a0, a1 = pieces(a)
    b0, b1 = pieces(b)
    return product(a0, b0) + (product(a0, b1) + product(a1, b0))


def dot_exact(table, b):
    table = table.astype(bf16)
    b0, b1 = pieces(b)
    return dot(table, b0) + dot(table, b1)


def traction(jump, normal, weight0, weight1):
    j0, j1, j2 = jump
    n0, n1, n2 = normal
    along = n0 * j0 + n1 * j1 + n2 * j2
    t0, t1, t2 = j0 - along * n0, j1 - along * n1, j2 - along * n2
    opening = along * along + shear_weight * (t0 * t0 + t1 * t1 + t2 * t2)
    beta = weight1 * jnp.exp(opening * (-1.0 / opening_scale))
    alpha = weight0 + beta
    gamma = beta * along
    return [alpha * j0 + gamma * n0, alpha * j1 + gamma * n1, alpha * j2 + gamma * n2]


def build_inner(links, geometry, weights, jac, coef, index):
    inverse = 1.0 / jac
    for q in range(3):
        geo = geometry(q)
        link = links(q)
        partner = link[0:1, :]
        state = link[1:2, :]
        scale = geo[3:4, :] * inverse
        coef[5 * q : 5 * q + 3, :] = geo[0:3, :]
        coef[5 * q + 3 : 5 * q + 4, :] = jnp.where(state == 0, scale, 0.0)
        coef[5 * q + 4 : 5 * q + 5, :] = jnp.where(state == 1, (1.0 - shear_weight) * scale, 0.0)
        index[q : q + 1, :] = lax.bitwise_and(partner, BLOCK - 1)
        index[3 + q : 4 + q, :] = lax.div(partner, BLOCK)
    count = weights.shape[0]
    coef[15 : 15 + count, :] = weights * inverse


def local_changes(field, starts, coef, index, ops):
    strain_op, pick, lift = ops
    blocks = strain_op.shape[0] // ROWS
    factors = []
    for at in starts:
        value = jnp.concatenate(
            [field[:, at : at + TILE], jnp.zeros((DEPTH - ROWS, TILE), f32)], axis=0
        )
        high, low = pieces(value)
        factors.append(jnp.concatenate([high, low, high], axis=0))
    traces = [dot(pick[...], factor[0 : 2 * DEPTH]) for factor in factors]
    strains = [dot(strain_op[...], factor) for factor in factors]
    forces = []
    for at, trace in zip(starts, traces):
        halves = []
        for half in range(TILE // BLOCK):
            lanes = slice(at + half * BLOCK, at + (half + 1) * BLOCK)
            part = trace[:, half * BLOCK : (half + 1) * BLOCK]
            rows = []
            for q in range(3):
                where = jnp.broadcast_to(index[q : q + 1, lanes], (TRACE, BLOCK))
                side = index[3 + q : 4 + q, lanes]
                found = [
                    jnp.take_along_axis(
                        part[k * TRACE : (k + 1) * TRACE], where, axis=1, mode="promise_in_bounds"
                    )
                    for k in range(3)
                ]
                paired = jnp.where(side == 0, found[0], jnp.where(side == 1, found[1], found[2]))
                jump = paired - part[q * TRACE : (q + 1) * TRACE]
                weights = [coef[5 * q + r : 5 * q + r + 1, lanes] for r in range(5)]
                rows += traction(split_rows(jump), weights[0:3], weights[3], weights[4])
            halves.append(jnp.concatenate(rows, axis=0))
        forces.append(jnp.concatenate(halves, axis=1))
    results = []
    for at, strain, force in zip(starts, strains, forces):
        high, low = pieces(force)
        total = dot(lift[...], jnp.concatenate([high, low, high], axis=0))
        parts = []
        for g in range(ROWS // 8):
            part = total[g * 8 : (g + 1) * 8]
            for m in range(blocks):
                first = (g * blocks + m) * 8
                part = part + coef[15 + m : 16 + m, at : at + TILE] * strain[first : first + 8]
            parts.append(part)
        results.append(jnp.concatenate(parts, axis=0))
    return results


def load_state(source, target):
    target[...] = jnp.zeros_like(target)
    for c in range(3):
        target[c * PAD : c * PAD + source.shape[1], :] = source[c]


def trace_of(field, lanes):
    return [field[c * PAD : c * PAD + FACE, lanes] for c in range(3)]


def pack(first, second, extra, shared, groups, places, upper, lower, cross):
    parts = [first]
    if second is not None:
        parts.append(second)
    if extra is not None:
        parts.append(extra)
    rows = jnp.concatenate(parts, axis=0)
    upper[...] = rows[:, 0:shared]
    lower[...] = rows[:, shared : 2 * shared]
    rest = rows[:, 2 * shared :]
    missing = BLOCK - rest.shape[0]
    rest = jnp.concatenate([rest, jnp.zeros((missing, rest.shape[1]), f32)], axis=0)
    blocks = rest.T.reshape(rest.shape[1] // 8, 8, BLOCK)
    group = lax.axis_index("group")
    cross[pl.ds(group * places, places)] = jnp.zeros((places, 8, BLOCK), f32)
    for b in range(groups - 1):
        target = lax.rem(group + (1 + b), groups)
        cross[pl.ds(target * places, places)] = blocks[b * places : (b + 1) * places]


def unpack(upper, lower, cross, groups, places, width):
    group = lax.axis_index("group")
    parts = []
    for b in range(groups - 1):
        source = lax.rem(group + (1 + b), groups)
        parts.append(cross[pl.ds(source * places, places)].reshape(places * 8, BLOCK))
    spare = width - (groups - 1) * places * 8
    if spare:
        parts.append(jnp.zeros((spare, BLOCK), f32))
    slots = jnp.concatenate(parts, axis=0).T
    return jnp.concatenate([upper[...], lower[...], slots[0 : upper.shape[0]]], axis=1)


def split_rows(value):
    return [value[c * FACE : (c + 1) * FACE] for c in range(3)]


def rim_traction(jump, rim):
    rows = [rim[r : r + 1, :] for r in range(5)]
    return jnp.concatenate(traction(split_rows(jump), rows[0:3], rows[3], rows[4]), axis=0)


def times_lift0(lift0, value):
    high, low = pieces(value)
    return dot(lift0[...], jnp.concatenate([high, low, high], axis=0))


def first_pack(sizes, disp, jac, upper, lower, cross):
    shared, groups, places, rim_lanes = sizes
    trace = jnp.concatenate([disp[c, 0:FACE, :] for c in range(3)], axis=0)
    extra = jnp.broadcast_to(1.0 / jac[:, 0:rim_lanes], (8, rim_lanes))
    pack(trace, None, extra, shared, groups, places, upper, lower, cross)


def prepare(
    strain,
    face_mass,
    mass_inverse,
    place,
    lift,
    lift0,
    strain_op,
    lift_op,
    lift0_op,
    trace_op,
    wide,
    corner,
    inverse,
    first,
    second,
):
    nodes = mass_inverse.shape[0]
    size = 3 * nodes
    count = strain.shape[1]
    blocks = count // size
    wide[...] = jnp.zeros_like(wide)
    corner[...] = jnp.zeros_like(corner)
    corner[0:nodes, 0:nodes] = (time_step * time_step) * mass_inverse[...]
    inverse[...] = jnp.zeros_like(inverse)
    for c in range(3):
        wide[c * PAD : c * PAD + nodes, 0:count] = strain[c * nodes : (c + 1) * nodes, :]
        inverse[c * PAD : (c + 1) * PAD, :] = pltpu.roll(corner[...], c * PAD, 1)
    rows0, rows1 = pieces(wide[...])
    base = inverse[...]
    base0, base1 = pieces(base)
    left = dot(base0, rows0) + (dot(base0, rows1) + dot(base1, rows0))
    left0, left1 = pieces(left)
    for m in range(blocks):
        begin = m * size // DEPTH * DEPTH
        end = min(begin + 2 * DEPTH, wide.shape[1])
        lane = begin + lax.broadcasted_iota(jnp.int32, (DEPTH, end - begin), 1)
        inside = (lane >= m * size) & (lane < (m + 1) * size)
        cut0 = jnp.where(inside, left[:, begin:end], 0.0)
        cut0, cut1 = pieces(cut0)
        value = -(
            dot_t(cut0, rows0[:, begin:end])
            + (dot_t(cut0, rows1[:, begin:end]) + dot_t(cut1, rows0[:, begin:end]))
        )
        high = value.astype(bf16).astype(f32)
        low = value - high
        for g in range(ROWS // 8):
            at = (g * blocks + m) * 8
            first[at : at + 8, :] = high[g * 8 : (g + 1) * 8]
            second[at : at + 8, :] = low[g * 8 : (g + 1) * 8]
    high = first[...].astype(bf16)
    strain_op[:, 0:DEPTH] = high
    strain_op[:, DEPTH : 2 * DEPTH] = high
    strain_op[:, 2 * DEPTH :] = second[...].astype(bf16)

    row = lax.broadcasted_iota(jnp.int32, (3 * TRACE, 9 * TRACE), 0)
    col = lax.broadcasted_iota(jnp.int32, (3 * TRACE, 9 * TRACE), 1)
    part0, part1 = pieces(dot_exact(place[0 : 3 * TRACE, :], face_mass[...]))
    spread = place[...].astype(bf16)
    mass = dot_t(part0, spread) + dot_t(part1, spread)
    same = lax.rem(lax.div(row, FACE), 3) == lax.rem(lax.div(col, FACE), 3)
    mass = jnp.where(same, mass, 0.0)
    each = jnp.where(lax.div(row, TRACE) == lax.rem(lax.div(col, TRACE), 3), mass, 0.0)
    zeros = jnp.zeros((DEPTH - ROWS, 9 * TRACE), f32)

    def lifted(table, factor):
        value = jnp.concatenate([dot_exact(table[...], factor), zeros[:, 0 : factor.shape[1]]], axis=0)
        return dot_pieces(base, value)[0:ROWS]

    def three(value):
        high = value.astype(bf16).astype(f32)
        col = lax.broadcasted_iota(jnp.int32, value.shape, 1)
        return jnp.where(col < value.shape[1] // 3 * 2, high, value - high).astype(bf16)

    lift_op[...] = three(lifted(lift, each))
    value = lifted(lift0, mass[0:TRACE, 0 : 3 * TRACE])
    lift0_op[...] = three(value)
    trace_op[...] = three(
        jnp.concatenate([value[c * PAD : c * PAD + FACE] for c in range(3)], axis=0)
    )


def start_rim(
    sizes,
    disp,
    vel,
    links,
    geometry,
    weights,
    jac,
    next_links,
    next_geometry,
    cross_links,
    cross_geometry,
    strain_op,
    pick,
    lift_op,
    field_out,
    vel_out,
    coef,
    index,
    rim,
):
    shared, groups, places, lanes = sizes
    elements = links.shape[1] // 3
    inverse = jac[:, 0:lanes]
    build_inner(
        lambda q: links[:, q * elements : q * elements + lanes],
        lambda q: geometry[:, q * elements : q * elements + lanes],
        weights[:, 0:lanes],
        inverse,
        coef,
        index,
    )
    rim[...] = jnp.zeros_like(rim)
    slots = cross_links.shape[1]
    for at, count, geo, state in (
        (0, shared, next_geometry[0:4, :], next_links[0:1, :]),
        (shared, shared, next_geometry[4:8, :], next_links[1:2, :]),
        (2 * shared, slots, cross_geometry[...], cross_links[...]),
    ):
        rim[0:3, at : at + count] = geo[0:3, :]
        rim[3:4, at : at + count] = jnp.where(state == 0, 1.0, 0.0)
        rim[4:5, at : at + count] = jnp.where(state == 1, 1.0 - shear_weight, 0.0)
        rim[6:7, at : at + count] = geo[3:4, :]
    rim[5:6, :] = rim[6:7, :] * (1.0 / inverse)
    load_state(disp, field_out)
    load_state(vel, vel_out)
    ops = (strain_op, pick, lift_op)
    starts = range(0, lanes, TILE)
    for at, change in zip(starts, local_changes(field_out, starts, coef, index, ops)):
        span = pl.ds(at, TILE)
        vel_out[:, span] = time_step * vel_out[:, span] + change


def first_step(
    sizes,
    upper_in,
    lower_in,
    cross_in,
    field,
    vel,
    coef,
    index,
    rim,
    strain_op,
    pick,
    lift_op,
    lift0_op,
    field_out,
    vel_out,
    own_out,
    rim_out,
    upper,
    lower,
    cross,
):
    shared, groups, places, lanes = sizes
    every = slice(None)
    arrived = unpack(upper_in, lower_in, cross_in, groups, places, lanes - 2 * shared)
    own = jnp.concatenate(trace_of(field, every), axis=0)
    pull = rim_traction(arrived[0:TRACE] - own, rim)
    rim_out[0:6, :] = rim[0:6, :]
    rim_out[6:7, :] = rim[5:6, :] + rim[6:7, :] * arrived[TRACE : TRACE + 1]
    rim_out[7:8, :] = rim[7:8, :]
    change = times_lift0(lift0_op, pull * rim[5:6, :])
    speed = vel[...] + change
    vel_out[...] = speed
    field_out[...] = field[...] + speed
    send_two(sizes, field_out, vel_out, own_out, coef, index, (strain_op, pick, lift_op), upper, lower, cross)


def send_two(sizes, field_out, vel_out, own_out, coef, index, ops, upper, lower, cross):
    shared, groups, places, lanes = sizes
    every = slice(None)
    first = jnp.concatenate(trace_of(field_out, every), axis=0)
    own_out[...] = first
    starts = range(0, lanes, TILE)
    for at, change in zip(starts, local_changes(field_out, starts, coef, index, ops)):
        span = pl.ds(at, TILE)
        speed = vel_out[:, span] + change
        vel_out[:, span] = speed
        field_out[:, span] = field_out[:, span] + speed
    second = jnp.concatenate(trace_of(field_out, every), axis=0)
    pack(first, second, None, shared, groups, places, upper, lower, cross)


def take_two(sizes, upper_in, lower_in, cross_in, field, vel, own, coef, index, rim, ops, lift0_op, trace_op, field_out, vel_out):
    shared, groups, places, lanes = sizes
    every = slice(None)
    arrived = unpack(upper_in, lower_in, cross_in, groups, places, lanes - 2 * shared)
    pull = rim_traction(arrived[0:TRACE] - own[...], rim)
    later = arrived[TRACE : 2 * TRACE] - jnp.concatenate(trace_of(field, every), axis=0)
    later = later - times_lift0(trace_op, pull * rim[6:7, :])
    pull_later = rim_traction(later, rim)
    change = times_lift0(lift0_op, pull * rim[5:6, :])
    vel_out[...] = vel[...] + change
    field_out[...] = field[...] + change
    later = times_lift0(lift0_op, pull_later * rim[5:6, :])
    starts = range(0, lanes, TILE)
    for at, change in zip(starts, local_changes(field_out, starts, coef, index, ops)):
        span = pl.ds(at, TILE)
        speed = vel_out[:, span] + (change + later[:, at : at + TILE])
        vel_out[:, span] = speed
        field_out[:, span] = field_out[:, span] + speed


def middle_steps(
    sizes,
    upper_in,
    lower_in,
    cross_in,
    field,
    vel,
    own,
    coef,
    index,
    rim,
    strain_op,
    pick,
    lift_op,
    lift0_op,
    trace_op,
    *rest,
):
    field_out, vel_out, own_out, upper, lower, cross = rest[-6:]
    ops = (strain_op, pick, lift_op)
    take_two(sizes, upper_in, lower_in, cross_in, field, vel, own, coef, index, rim, ops, lift0_op, trace_op, field_out, vel_out)
    send_two(sizes, field_out, vel_out, own_out, coef, index, ops, upper, lower, cross)


def last_steps(
    sizes,
    upper_in,
    lower_in,
    cross_in,
    field,
    vel,
    own,
    coef,
    index,
    rim,
    strain_op,
    pick,
    lift_op,
    lift0_op,
    trace_op,
    *rest,
):
    disp_out, vel_out, field_new, vel_new = rest[-4:]
    ops = (strain_op, pick, lift_op)
    take_two(sizes, upper_in, lower_in, cross_in, field, vel, own, coef, index, rim, ops, lift0_op, trace_op, field_new, vel_new)
    store_state(field_new, vel_new, disp_out, vel_out)


def store_state(field, vel, disp_out, vel_out):
    for c in range(3):
        nodes = disp_out.shape[1]
        disp_out[c] = field[c * PAD : c * PAD + nodes, :]
        vel_out[c] = (1.0 / time_step) * vel[c * PAD : c * PAD + nodes, :]


def advance(steps, field, speed, coef, index, ops):
    starts = range(0, field.shape[1], TILE)

    def step(_, carry):
        for at, change in zip(starts, local_changes(field, starts, coef, index, ops)):
            span = pl.ds(at, TILE)
            new = speed[:, span] + change
            speed[:, span] = new
            field[:, span] = field[:, span] + new
        return carry

    lax.fori_loop(0, steps, step, 0)


def inside_first(
    steps,
    disp,
    vel,
    link1,
    link2,
    link3,
    geo1,
    geo2,
    geo3,
    weights,
    jac,
    strain_op,
    pick,
    lift_op,
    after,
    field,
    speed,
    coef,
    index,
):
    links = (link1, link2, link3)
    geos = (geo1, geo2, geo3)
    build_inner(
        lambda q: links[q][...], lambda q: geos[q][...], weights[...], jac[...], coef, index
    )
    load_state(disp, field)
    load_state(vel, speed)
    speed[...] = time_step * speed[...]
    advance(steps, field, speed, coef, index, (strain_op, pick, lift_op))


def inside_last(
    steps, field_in, speed_in, coef, index, strain_op, pick, lift_op, after, disp_out, vel_out, field, speed
):
    field[...] = field_in[...]
    speed[...] = speed_in[...]
    advance(steps, field, speed, coef, index, (strain_op, pick, lift_op))
    store_state(field, speed, disp_out, vel_out)


def struct(shape, dtype=f32):
    return jax.ShapeDtypeStruct(shape, dtype)


def cost(flops):
    return pl.CostEstimate(flops=flops, bytes_accessed=1 << 20, transcendentals=0)


def shifted(value, axis, steps):
    count = lax.axis_size(axis)
    pairs = [(source, (source + steps) % count) for source in range(count)]
    return lax.ppermute(value, axis, pairs)


def exchange(upper, lower, cross):
    mixed = lax.all_to_all(cross, ("group", "sub"), 0, 0, tiled=True)
    return shifted(lower, "sub", -1), shifted(upper, "sub", 1), mixed


def shards(
    displacement,
    velocity,
    geometry_weights,
    jacobian,
    strain_map,
    face_mass,
    mass_inverse,
    local_links,
    local_geometry,
    neighbour_links,
    neighbour_geometry,
    cross_links,
    cross_geometry,
):
    components, nodes, elements = displacement.shape
    count = geometry_weights.shape[0]
    groups = lax.axis_size("group")
    places = lax.axis_size("sub")
    slots = cross_links.shape[0]
    shared = neighbour_links.shape[1]
    lanes = math.ceil((2 * shared + slots) / TILE) * TILE
    sizes = (shared, groups, places, lanes)
    place, lift, lift0, pick = (jnp.asarray(t) for t in tables())
    pick = pick.astype(bf16)
    jac = jacobian.reshape(1, elements)
    cross_row = cross_links.reshape(1, slots)
    state_shape = struct((ROWS, lanes))
    vmem = pl.BlockSpec(memory_space=pltpu.VMEM)
    anywhere = pl.BlockSpec(memory_space=pl.ANY)
    part = pl.BlockSpec((components, nodes, lanes), lambda i: (0, 0, 0))
    devices = groups * places
    params = pltpu.CompilerParams(vmem_limit_bytes=VMEM_LIMIT)

    def messages(height):
        return (struct((height, shared)), struct((height, shared)), struct((devices, 8, BLOCK)))

    sends = pl.pallas_call(
        functools.partial(first_pack, sizes),
        grid=(1,),
        out_shape=messages(TRACE + 8),
        in_specs=[part, vmem],
        cost_estimate=cost(1 << 20),
        compiler_params=params,
        name="first_pack",
    )(displacement, jac)
    arrived = exchange(*sends)

    wide = math.ceil(strain_map.shape[0] / DEPTH) * DEPTH
    strain_op, lift_op, lift0_op, trace_op = pl.pallas_call(
        prepare,
        out_shape=(
            struct((count * ROWS, 3 * DEPTH), bf16),
            struct((ROWS, 9 * TRACE), bf16),
            struct((ROWS, 3 * TRACE), bf16),
            struct((TRACE, 3 * TRACE), bf16),
        ),
        scratch_shapes=[
            pltpu.VMEM((DEPTH, wide), f32),
            pltpu.VMEM((PAD, DEPTH), f32),
            pltpu.VMEM((DEPTH, DEPTH), f32),
            pltpu.VMEM((count * ROWS, DEPTH), f32),
            pltpu.VMEM((count * ROWS, DEPTH), f32),
        ],
        cost_estimate=cost(1 << 24),
        compiler_params=params,
        name="prepare",
    )(strain_map.T, face_mass, mass_inverse, place, lift, lift0)
    ops = (strain_op, pick, lift_op)

    field, vel, coef, index, rim = pl.pallas_call(
        functools.partial(start_rim, sizes),
        grid=(1,),
        out_shape=(
            state_shape,
            state_shape,
            struct((24, lanes)),
            struct((8, lanes), jnp.int32),
            struct((8, lanes)),
        ),
        in_specs=[part, part] + [vmem] * 11,
        cost_estimate=cost(1 << 24),
        compiler_params=params,
        name="start_rim",
    )(
        displacement,
        velocity,
        local_links,
        local_geometry,
        geometry_weights,
        jac,
        neighbour_links,
        neighbour_geometry,
        cross_row,
        cross_geometry,
        *ops,
    )

    field, vel, own, rim, *sends = pl.pallas_call(
        functools.partial(first_step, sizes),
        out_shape=(state_shape, state_shape, struct((TRACE, lanes)), struct((8, lanes)))
        + messages(2 * TRACE),
        cost_estimate=cost(1 << 24),
        compiler_params=params,
        name="first_step",
    )(*arrived, field, vel, coef, index, rim, *ops, lift0_op)
    arrived = exchange(*sends)

    inner = elements - lanes
    outputs = []
    waits = []
    if inner:
        width = math.gcd(lanes, inner)
        skip = lanes // width
        per_face = elements // width
        piece = pl.BlockSpec((components, nodes, width), lambda i: (0, 0, skip + i))

        def columns(height, q=0):
            return pl.BlockSpec((height, width), lambda i: (0, q * per_face + skip + i))

        def inner_columns(height):
            return pl.BlockSpec((height, width), lambda i: (0, i))

        inner_state = [
            (ROWS, f32),
            (ROWS, f32),
            (24, f32),
            (8, jnp.int32),
        ]
        state = pl.pallas_call(
            functools.partial(inside_first, 3),
            grid=(inner // width,),
            out_shape=[struct((height, inner), kind) for height, kind in inner_state],
            in_specs=[piece, piece]
            + [columns(2, q) for q in range(3)]
            + [columns(4, q) for q in range(3)]
            + [columns(count), columns(1)]
            + [vmem] * 3
            + [anywhere],
            out_specs=[inner_columns(height) for height, kind in inner_state],
            cost_estimate=cost(1 << 26),
            compiler_params=params,
            name="inside_first",
        )(
            displacement,
            velocity,
            *[local_links] * 3,
            *[local_geometry] * 3,
            geometry_weights,
            jac,
            *ops,
            own,
        )
        waits = [state[0]]

    field, vel, own, *sends = pl.pallas_call(
        functools.partial(middle_steps, sizes),
        out_shape=(state_shape, state_shape, struct((TRACE, lanes))) + messages(2 * TRACE),
        in_specs=[vmem] * 14 + [anywhere] * len(waits),
        cost_estimate=cost(1 << 24),
        compiler_params=params,
        name="middle_steps",
    )(*arrived, field, vel, own, coef, index, rim, *ops, lift0_op, trace_op, *waits)
    arrived = exchange(*sends)

    if inner:
        outputs = pl.pallas_call(
            functools.partial(inside_last, 2),
            grid=(inner // width,),
            out_shape=(struct(displacement.shape), struct(displacement.shape)),
            in_specs=[inner_columns(height) for height, kind in inner_state]
            + [vmem] * 3
            + [anywhere],
            out_specs=(piece, piece),
            scratch_shapes=[pltpu.VMEM((ROWS, width), f32), pltpu.VMEM((ROWS, width), f32)],
            cost_estimate=cost(1 << 26),
            compiler_params=params,
            name="inside_last",
        )(*state, *ops, own)

    return pl.pallas_call(
        functools.partial(last_steps, sizes),
        grid=(1,),
        out_shape=(struct(displacement.shape), struct(displacement.shape)),
        in_specs=[vmem] * 14 + [anywhere] * len(outputs),
        out_specs=(part, part),
        scratch_shapes=[pltpu.VMEM((ROWS, lanes), f32), pltpu.VMEM((ROWS, lanes), f32)],
        input_output_aliases={14: 0, 15: 1} if inner else {},
        cost_estimate=cost(1 << 24),
        compiler_params=params,
        name="last_steps",
    )(*arrived, field, vel, own, coef, index, rim, *ops, lift0_op, trace_op, *outputs)


def solution(mesh):
    return jax.shard_map(
        shards,
        mesh=mesh,
        in_specs=(
            P(None, None, ("group", "sub")),
            P(None, None, ("group", "sub")),
            P(None, ("group", "sub")),
            P(("group", "sub")),
            P(),
            P(),
            P(),
            P(None, ("group", "sub")),
            P(None, ("group", "sub")),
            P(None, ("group", "sub")),
            P(None, ("group", "sub")),
            P(("group", "sub")),
            P(None, ("group", "sub")),
        ),
        out_specs=(P(None, None, ("group", "sub")), P(None, None, ("group", "sub"))),
        check_vma=False,
    )
```
